128 devices in a mesh: fsdp: 32 (over z, x, core), tp: 4 (over y).
Axes of the slice: x: 4, y: 4, z: 4, core: 2. Of those that a mesh axis runs over, the one named last changes fastest.
Arguments:
- gradients: bfloat16 [2, 8192, 8192], P(None, 'fsdp', 'tp'), may hold values from -120 to 120
- row_counts: int32 [32], replicated, may hold values from 128 to 256, as said below
- block_owner: int32 [2, 8], replicated, may hold values from 0 to 31, as said below
Outputs:
- update: bfloat16 [2, 8192, 8192], P(None, 'fsdp', 'tp')
- owned: bfloat16 [32768, 4096], P('fsdp', 'tp')
The draws below stay inside these ranges and needn't reach their ends.
Inputs may be any that keep to these rules, and one draw needn't show every extreme that they name: `row_counts`: every count is a multiple of 128; some index holds exactly 256. `block_owner`: blocks whose columns lie on the same tp index have distinct owners.
All inputs are finite; a program needn't handle non-finite values.
Results may differ from the reference program's by a relative error of at most 0.005.
The reference program's roundings to bfloat16 on the way count: a program that leaves them out, or rounds other values in their place, can miss the bound.
Values may be sent and summed in bfloat16 or wider, within the bound.
No kernel may reach another device: no remote copies, remote signals or barrier semaphores. Data moves between devices by JAX's collectives and lax.ppermute only.
A program may use at most 128 MiB of HBM per device.

```python
import jax
import jax.numpy as jnp
from jax import lax

D = 8192
BLOCK = 1024
GRAIN = 128
LAYERS = 2
ROW_CAP = 256
ROWS = 8192
N_FSDP = 32
N_TP = 4


group_width = 32


def draw_gradients(key, part):
    keys = jax.random.split(jax.random.fold_in(key, 7), 6)
    group_total = D // group_width
    per_block = BLOCK // group_width
    member_list = []
    for block_index in range(D // BLOCK):
        shuffled = jax.random.permutation(jax.random.fold_in(keys[5], 40 + block_index), BLOCK)
        member_list.append(shuffled % per_block + block_index * per_block)
    membership = jnp.concatenate(member_list).astype(jnp.int32)
    independent = jnp.clip(jax.random.normal(keys[0], (LAYERS, ROWS, D), jnp.float32), -4.0, 4.0)
    common = jnp.clip(jax.random.normal(keys[1], (LAYERS, ROWS, group_total), jnp.float32), -4.0, 4.0)
    row_scale = jnp.exp(jax.random.uniform(keys[2], (LAYERS, ROWS, 1), jnp.float32, -1.15, 1.15))
    group_scale = jnp.exp(jax.random.uniform(keys[3], (LAYERS, 1, group_total), jnp.float32, -1.15, 1.15))
    spread_common = jnp.take(common, membership, axis=2)
    col_scale = jnp.take(group_scale, membership, axis=2)
    noise = 0.4 * independent + 0.92 * spread_common
    return (noise * row_scale * col_scale).astype(jnp.bfloat16)


def draw_row_counts(key, part):
    keys = jax.random.split(jax.random.fold_in(key, 19), 2)
    grains = jax.random.randint(keys[0], (N_FSDP,), 1, ROW_CAP // GRAIN + 1)
    fullest = jax.random.randint(keys[1], (), 0, N_FSDP)
    return jnp.where(jnp.arange(N_FSDP) == fullest, ROW_CAP, grains * GRAIN).astype(jnp.int32)


def draw_block_owner(key, part):
    per_group = D // (BLOCK * N_TP)
    columns = []
    for tp_group in range(N_TP):
        shuffled = jax.random.permutation(jax.random.fold_in(key, 300 + tp_group), N_FSDP)
        columns.append(shuffled[:LAYERS * per_group].reshape(LAYERS, per_group))
    return jnp.concatenate(columns, axis=1).astype(jnp.int32)


def setup_inputs(seed: int = 0) -> dict:
    key_list = jax.random.split(jax.random.key(seed), 4)
    gradients = draw_gradients(jax.random.fold_in(key_list[3], 71), 0)
    row_counts = draw_row_counts(jax.random.fold_in(key_list[3], 71), 0)
    block_owner = draw_block_owner(jax.random.fold_in(key_list[3], 71), 0)
    return {"gradients": gradients, "row_counts": row_counts, "block_owner": block_owner}


damping = 0.01

def newton_root(statistic):
    identity = jnp.eye(statistic.shape[0], dtype=jnp.float32)
    scaling = 2.5 / jnp.sqrt(jnp.sum(statistic * statistic))
    scaled = scaling * statistic
    factor_one = (5.0 * identity - scaled) / 4.0
    square = jnp.dot(factor_one, factor_one, precision=lax.Precision.HIGHEST)
    inner_part = jnp.dot(square, scaled, precision=lax.Precision.HIGHEST)
    contracted = jnp.dot(square, inner_part, precision=lax.Precision.HIGHEST)
    factor_two = (5.0 * identity - contracted) / 4.0
    result = jnp.dot(jnp.sqrt(jnp.sqrt(scaling)) * factor_one, factor_two, precision=lax.Precision.HIGHEST)
    return result.astype(jnp.bfloat16)

def gram_block(piece):
    widened = piece.astype(jnp.float32)
    return jnp.dot(widened.T, widened, precision=lax.Precision.HIGHEST)

def apply_block(paired):
    piece, root_block = paired
    return jnp.dot(piece, root_block, preferred_element_type=jnp.float32).astype(jnp.bfloat16)

def reference(gradients, row_counts, block_owner):
    positions = jnp.arange(ROWS, dtype=jnp.int32)
    limits = row_counts[positions // ROW_CAP]
    valid_rows = (positions % ROW_CAP < limits).astype(jnp.bfloat16)
    masked = gradients * valid_rows[None, :, None]
    total_rows = jnp.sum(row_counts).astype(jnp.float32)
    block_count = D // BLOCK
    per_group = block_count // N_TP
    identity = jnp.eye(BLOCK, dtype=jnp.float32)
    updates = []
    owned = jnp.zeros((N_FSDP, N_TP, BLOCK, BLOCK), jnp.bfloat16)
    for layer in range(LAYERS):
        blocked = jnp.transpose(masked[layer].reshape(ROWS, block_count, BLOCK), (1, 0, 2))
        grams = lax.map(gram_block, blocked)
        statistic = grams / total_rows + damping * identity
        root_list = lax.map(newton_root, statistic)
        applied = lax.map(apply_block, (blocked, root_list))
        updates.append(jnp.transpose(applied, (1, 0, 2)).reshape(ROWS, D))
        for column in range(block_count):
            owned = owned.at[block_owner[layer, column], column // per_group].set(root_list[column])
    owned_flat = jnp.transpose(owned, (0, 2, 1, 3)).reshape(N_FSDP * BLOCK, N_TP * BLOCK)
    return (jnp.stack(updates), owned_flat)
```

```python
import jax
import jax.numpy as jnp
from jax import lax
from jax.experimental import pallas as pl
from jax.experimental.pallas import tpu as pltpu
from jax.sharding import Mesh, PartitionSpec as P

BLOCK = 1024
TILE = 128
HALF = 64
WIDE = 640
SIDE = 4
damping = 0.01
F32 = jnp.float32
BF16 = jnp.bfloat16
VMEM = pltpu.CompilerParams(vmem_limit_bytes=56 * 1024 * 1024)


def masked_rows(own, other, own_limit, other_limit):
    rows = lax.broadcasted_iota(jnp.int32, own.shape, 0)
    zero = jnp.zeros_like(own)
    return jnp.where(rows < own_limit, own, zero), jnp.where(rows < other_limit, other, zero)


def gram_kernel(scalars, own, other, *refs):
    outs, (wide, gram) = refs[:8], refs[8:]
    z, x = scalars[1], scalars[2]
    rows = own.shape[1]
    own_value, other_value = masked_rows(own[0], other[...], scalars[3], scalars[4])
    for block in range(2):
        columns = slice(block * BLOCK, (block + 1) * BLOCK)
        wide[:rows, :BLOCK] = own_value[:, columns]
        wide[rows:, :BLOCK] = other_value[:, columns]
        wide[:, BLOCK:] = wide[:, : BLOCK // 2]
        for pair in range(4):
            start = pair * 2 * TILE
            part = lax.dot_general(
                wide[:, start : start + 2 * TILE],
                wide[:, start : start + 6 * TILE],
                (((0,), (0,)), ((), ())),
                preferred_element_type=F32,
            )
            for quarter in range(4):
                shift = TILE * (quarter // 2)
                gram[4 * pair + quarter] = part[
                    quarter * HALF : (quarter + 1) * HALF, shift : shift + WIDE
                ]
        for first in range(SIDE):
            for second in range(SIDE):
                if block == 0:
                    chunk = ((z + second) % SIDE) * SIDE + (x + first) % SIDE
                else:
                    chunk = ((z + first) % SIDE) * SIDE + (x + second) % SIDE
                target = outs[4 * block + first]
                target[second] = gram[chunk].astype(target.dtype)


def first_sum_kernel(*refs):
    ins, outs = refs[:8], refs[8:]
    for side in range(2):
        group = ins[4 * side : 4 * side + 4]
        for second in range(SIDE):
            value = group[0][second]
            for k in range(1, SIDE):
                value = value + group[k][second].astype(F32)
            target = outs[4 * side + second]
            target[...] = value.astype(target.dtype)


def second_sum_kernel(*refs):
    ins, outs = refs[:8], refs[8:]
    for side in range(2):
        group = ins[4 * side : 4 * side + 4]
        value = group[0][...]
        for k in range(1, SIDE):
            value = value + group[k][...].astype(F32)
        outs[side][...] = value.astype(BF16)


def root_kernel(scalars, inverse_rows, own, other, *refs):
    sets, outs, scratch = refs[:8], refs[8:12], refs[12:]
    update_own, update_other, root_own, root_other = outs
    s_ref, w_ref, v_ref, sb_ref, rb_ref, wb_ref = scratch
    block = pl.program_id(0)
    z, x = scalars[1], scalars[2]

    def assemble(group, along_x):
        for first in range(SIDE):
            for second in range(SIDE):
                if along_x:
                    chunk = ((z + second) % SIDE) * SIDE + (x + first) % SIDE
                else:
                    chunk = ((z + first) % SIDE) * SIDE + (x + second) % SIDE
                row = pl.multiple_of(chunk * HALF, HALF)
                slab = chunk // 2
                value = group[first][second].astype(F32)
                for k in range(WIDE // TILE):
                    column = pl.multiple_of(((slab + k) % 8) * TILE, TILE)
                    s_ref[pl.ds(row, HALF), pl.ds(column, TILE)] = value[
                        :, k * TILE : (k + 1) * TILE
                    ]

    @pl.when(block == 0)
    def _():
        assemble(sets[:4], True)
        root_own[...] = jnp.zeros_like(root_own)
        root_other[...] = jnp.zeros_like(root_other)

    @pl.when(block == 1)
    def _():
        assemble(sets[4:], False)

    for slab in range(8):
        for k in range(1, 4):
            far = (slab + k) % 8
            here = slice(slab * TILE, (slab + 1) * TILE)
            there = slice(far * TILE, (far + 1) * TILE)
            s_ref[there, here] = s_ref[here, there].T

    def diagonal(start, rows):
        row = lax.broadcasted_iota(jnp.int32, (rows, BLOCK), 0) + start
        return row == lax.broadcasted_iota(jnp.int32, (rows, BLOCK), 1)

    scale = inverse_rows[0]
    total = jnp.zeros((1, BLOCK), F32)
    for slab in range(8):
        here = slice(slab * TILE, (slab + 1) * TILE)
        value = s_ref[here, :] * scale
        value = value + jnp.where(diagonal(slab * TILE, TILE), damping, 0.0)
        s_ref[here, :] = value
        total = total + jnp.sum(value * value, axis=0, keepdims=True)
    norm = jnp.sum(total, axis=1, keepdims=True)
    scaling = 2.5 / jnp.sqrt(norm)
    for slab in range(8):
        here = slice(slab * TILE, (slab + 1) * TILE)
        value = s_ref[here, :] * scaling
        s_ref[here, :] = value
        sb_ref[here, :] = value.astype(BF16)
    step = 256
    for part in range(BLOCK // step):
        here = slice(part * step, (part + 1) * step)
        square = jnp.dot(sb_ref[here, :], sb_ref[...], preferred_element_type=F32)
        value = s_ref[here, :]
        rb_ref[here, :] = ((10.0 * value - square) * (1.0 / 16.0)).astype(BF16)
        inner = (5.0 * value - square) * 0.25
        w_ref[here, :] = inner
        wb_ref[here, :] = inner.astype(BF16)
    for part in range(BLOCK // step):
        here = slice(part * step, (part + 1) * step)
        product = jnp.dot(rb_ref[here, :], wb_ref[...], preferred_element_type=F32)
        inner = (25.0 / 16.0) * w_ref[here, :] - product
        v_ref[here, :] = inner
        sb_ref[here, :] = inner.astype(BF16)
    quarter = jnp.sqrt(jnp.sqrt(scaling))
    for part in range(BLOCK // step):
        here = slice(part * step, (part + 1) * step)
        product = jnp.dot(rb_ref[here, :], sb_ref[...], preferred_element_type=F32)
        inner = (25.0 / 16.0) * v_ref[here, :] - product
        factor = jnp.where(diagonal(part * step, step), 1.25, 0.0) - 0.25 * s_ref[here, :]
        wb_ref[here, :] = (quarter * ((5.0 * factor - inner) * 0.25)).astype(BF16)

    own_value, other_value = masked_rows(own[0], other[...], scalars[3], scalars[4])
    root = wb_ref[...]
    update_own[...] = jnp.dot(own_value, root, preferred_element_type=F32).astype(BF16)
    update_other[...] = jnp.dot(other_value, root, preferred_element_type=F32).astype(BF16)

    @pl.when(scalars[5] == block)
    def _():
        root_own[...] = wb_ref[...]

    @pl.when(scalars[6] == block)
    def _():
        root_other[...] = wb_ref[...]


def shifted(value, axis, distance):
    return lax.ppermute(value, axis, [(k, (k + distance) % SIDE) for k in range(SIDE)])


def swapped(value):
    return lax.ppermute(value, "core", [(0, 1), (1, 0)])


def body(gradients, row_counts, block_owner):
    z, x, core = (lax.axis_index(name).astype(jnp.int32) for name in ("z", "x", "core"))
    tp_index = lax.axis_index("tp")
    _, row_slots, columns = gradients.shape
    per_device = columns // BLOCK
    index = (z * SIDE + x) * 2 + core
    partner = index + 1 - 2 * core
    total_rows = jnp.sum(row_counts).astype(F32)
    inverse_rows = (1.0 / total_rows).reshape(1)
    local_owner = lax.dynamic_slice(block_owner, (core, tp_index * per_device), (1, per_device))[0]
    position = jnp.arange(per_device, dtype=jnp.int32)
    mine = jnp.max(jnp.where(local_owner == index, position, -1))
    theirs = jnp.max(jnp.where(local_owner == partner, position, -1))
    scalars = jnp.stack(
        [core, z, x, row_counts[index], row_counts[partner], mine, theirs]
    ).astype(jnp.int32)

    away = jnp.where(core == 0, gradients[1], gradients[0])
    other = swapped(away)

    chunk4 = (SIDE, HALF, WIDE)
    chunk1 = (HALF, WIDE)
    in_vmem = pl.BlockSpec(memory_space=pltpu.VMEM)
    packed = pl.pallas_call(
        gram_kernel,
        grid_spec=pltpu.PrefetchScalarGridSpec(
            num_scalar_prefetch=1,
            grid=(1,),
            in_specs=[
                pl.BlockSpec((1, row_slots, columns), lambda i, s: (s[0], 0, 0)),
                pl.BlockSpec((row_slots, columns), lambda i, s: (0, 0)),
            ],
            out_specs=[pl.BlockSpec(chunk4, lambda i, s: (0, 0, 0))] * 8,
            scratch_shapes=[
                pltpu.VMEM((2 * row_slots, BLOCK + BLOCK // 2), BF16),
                pltpu.VMEM((16, HALF, WIDE), F32),
            ],
        ),
        out_shape=[jax.ShapeDtypeStruct(chunk4, F32 if k % 4 == 0 else BF16) for k in range(8)],
        compiler_params=VMEM,
        name="gram",
    )(scalars, gradients, other)

    axes = ("x", "z")
    received = list(packed)
    for side in range(2):
        for k in range(1, SIDE):
            received[4 * side + k] = shifted(packed[4 * side + k], axes[side], k)
    summed = pl.pallas_call(
        first_sum_kernel,
        in_specs=[in_vmem] * 8,
        out_specs=[in_vmem] * 8,
        out_shape=[jax.ShapeDtypeStruct(chunk1, F32 if k % 4 == 0 else BF16) for k in range(8)],
        compiler_params=VMEM,
        name="first_sum",
    )(*received)
    received = list(summed)
    for side in range(2):
        for k in range(1, SIDE):
            received[4 * side + k] = shifted(summed[4 * side + k], axes[1 - side], k)
    reduced = pl.pallas_call(
        second_sum_kernel,
        in_specs=[in_vmem] * 8,
        out_specs=[in_vmem] * 2,
        out_shape=[jax.ShapeDtypeStruct(chunk1, BF16)] * 2,
        compiler_params=VMEM,
        name="second_sum",
    )(*received)
    sets = []
    for side in range(2):
        line = [reduced[side]]
        for k in range(1, SIDE):
            line.append(shifted(reduced[side], axes[1 - side], -k))
        line = jnp.stack(line)
        sets.append(line)
        for k in range(1, SIDE):
            sets.append(shifted(line, axes[side], -k))

    whole = pl.BlockSpec(chunk4, lambda k, s: (0, 0, 0))
    update_own, update_other, root_own, root_other = pl.pallas_call(
        root_kernel,
        grid_spec=pltpu.PrefetchScalarGridSpec(
            num_scalar_prefetch=1,
            grid=(per_device,),
            in_specs=[
                pl.BlockSpec(memory_space=pltpu.SMEM),
                pl.BlockSpec((1, row_slots, BLOCK), lambda k, s: (s[0], 0, k)),
                pl.BlockSpec((row_slots, BLOCK), lambda k, s: (0, k)),
            ]
            + [whole] * 8,
            out_specs=[
                pl.BlockSpec((row_slots, BLOCK), lambda k, s: (0, k)),
                pl.BlockSpec((row_slots, BLOCK), lambda k, s: (0, k)),
                pl.BlockSpec((BLOCK, BLOCK), lambda k, s: (0, 0)),
                pl.BlockSpec((BLOCK, BLOCK), lambda k, s: (0, 0)),
            ],
            scratch_shapes=[pltpu.VMEM((BLOCK, BLOCK), F32)] * 3
            + [pltpu.VMEM((BLOCK, BLOCK), BF16)] * 3,
        ),
        out_shape=[
            jax.ShapeDtypeStruct((row_slots, columns), BF16),
            jax.ShapeDtypeStruct((row_slots, columns), BF16),
            jax.ShapeDtypeStruct((BLOCK, BLOCK), BF16),
            jax.ShapeDtypeStruct((BLOCK, BLOCK), BF16),
        ],
        compiler_params=VMEM,
        name="root",
    )(scalars, inverse_rows, gradients, other, *sets)

    update_back = swapped(update_other)
    root_back = swapped(root_other)
    update = jnp.stack(
        [
            jnp.where(core == 0, update_own, update_back),
            jnp.where(core == 0, update_back, update_own),
        ]
    )
    owned = jnp.where(mine >= 0, root_own, root_back)
    return update, owned


def solution(mesh):
    cores = Mesh(mesh.devices.reshape(SIDE, SIDE, 2, SIDE), ("z", "x", "core", "tp"))
    rows = ("z", "x", "core")
    return jax.shard_map(
        body,
        mesh=cores,
        in_specs=(P(None, rows, "tp"), P(), P()),
        out_specs=(P(None, rows, "tp"), P(rows, "tp")),
        check_vma=False,
    )
```

```python
import functools

import jax
import jax.numpy as jnp
from jax import lax
from jax.experimental import pallas as pl
from jax.experimental.pallas import tpu as pltpu
from jax.sharding import Mesh, PartitionSpec as P


BLOCK = 1024
TILE = 128
HALF = 64
WIDE = 640
SIDE = 4
STEP = 512
damping = 0.01
F32 = jnp.float32
BF16 = jnp.bfloat16


def params(mebibytes):
    return pltpu.CompilerParams(vmem_limit_bytes=mebibytes * 1024 * 1024)


RESIDENT = pl.BlockSpec(memory_space=pltpu.VMEM)
CHUNK = (HALF, WIDE)
LINE = (SIDE, HALF, WIDE)
Z, X, CORE, TP = range(4)


def masked_rows(place, counts, own, other):
    index = (place[Z] * SIDE + place[X]) * 2
    rows = lax.broadcasted_iota(jnp.int32, own.shape, 0)
    zero = jnp.zeros_like(own)
    own_limit = counts[index + place[CORE]]
    other_limit = counts[index + 1 - place[CORE]]
    return jnp.where(rows < own_limit, own, zero), jnp.where(rows < other_limit, other, zero)


def chunk_of(place, side, first, second):
    z, x = (second, first) if side == 0 else (first, second)
    return ((place[Z] + z) % SIDE) * SIDE + (place[X] + x) % SIDE


def gram_kernel(side, place, counts, own, other, *refs):
    outs, (wide, gram) = refs[:4], refs[4:]
    rows = own.shape[1]
    columns = slice(side * BLOCK, (side + 1) * BLOCK)
    own_value, other_value = masked_rows(place, counts, own[0], other[:, columns])
    wide[:rows, :BLOCK] = own_value
    wide[rows:, :BLOCK] = other_value
    wide[:, BLOCK:] = wide[:, : BLOCK // 2]
    for pair in range(4):
        start = pair * 2 * TILE
        part = lax.dot_general(
            wide[:, start : start + 2 * TILE],
            wide[:, start : start + 6 * TILE],
            (((0,), (0,)), ((), ())),
            preferred_element_type=F32,
        )
        for quarter in range(4):
            shift = TILE * (quarter // 2)
            gram[4 * pair + quarter] = part[
                quarter * HALF : (quarter + 1) * HALF, shift : shift + WIDE
            ]
    for first in range(SIDE):
        for second in range(SIDE):
            value = gram[chunk_of(place, side, first, second)]
            outs[first][second] = value.astype(outs[first].dtype)


def first_sum_kernel(*refs):
    ins, outs = refs[:4], refs[4:]
    for second in range(SIDE):
        value = ins[0][second]
        for k in range(1, SIDE):
            value = value + ins[k][second].astype(F32)
        outs[second][...] = value.astype(outs[second].dtype)


def second_sum_kernel(*refs):
    value = refs[0][...]
    for k in range(1, SIDE):
        value = value + refs[k][...].astype(F32)
    refs[4][...] = value.astype(BF16)


def line_kernel(*refs):
    for k in range(SIDE):
        refs[4][k] = refs[k][...]


def diagonal(start, rows):
    row = lax.broadcasted_iota(jnp.int32, (rows, BLOCK), 0) + start
    return row == lax.broadcasted_iota(jnp.int32, (rows, BLOCK), 1)


def root_kernel(side, place, counts, owners, *refs):
    sets, refs = refs[:4], refs[4:]
    if side == 1:
        before, refs = refs[0], refs[1:]
    root, refs = refs[0], refs[1:]
    if side == 1:
        (root_own, root_other), refs = refs[:2], refs[2:]
    g_ref, w_ref, v_ref, rb_ref, wb_ref, vb_ref = refs

    for first in range(SIDE):
        for second in range(SIDE):
            chunk = chunk_of(place, side, first, second)
            row = pl.multiple_of(chunk * HALF, HALF)
            value = sets[first][second]
            for k in range(WIDE // TILE):
                column = pl.multiple_of(((chunk // 2 + k) % 8) * TILE, TILE)
                g_ref[pl.ds(row, HALF), pl.ds(column, TILE)] = value[:, k * TILE : (k + 1) * TILE]

    for slab in range(8):
        for k in range(1, 4):
            far = (slab + k) % 8
            here = slice(slab * TILE, (slab + 1) * TILE)
            there = slice(far * TILE, (far + 1) * TILE)
            g_ref[there, here] = g_ref[here, there].T

    squares = jnp.zeros((1, BLOCK), F32)
    trace = jnp.zeros((1, TILE), F32)
    row = lax.broadcasted_iota(jnp.int32, (TILE, TILE), 0)
    corner = row == lax.broadcasted_iota(jnp.int32, (TILE, TILE), 1)
    for slab in range(8):
        here = slice(slab * TILE, (slab + 1) * TILE)
        value = g_ref[here, :].astype(F32)
        squares = squares + jnp.sum(value * value, axis=0, keepdims=True)
        value = jnp.where(corner, g_ref[here, here].astype(F32), 0.0)
        trace = trace + jnp.sum(value, axis=0, keepdims=True)
    squares = jnp.sum(squares, axis=1, keepdims=True)
    trace = jnp.sum(trace, axis=1, keepdims=True)
    total = counts[0]
    for k in range(1, counts.shape[0]):
        total = total + counts[k]
    inverse = 1.0 / jnp.full((1, 1), total, jnp.int32).astype(F32)
    norm = squares * inverse * inverse + 2.0 * damping * inverse * trace
    scaling = 2.5 / jnp.sqrt(norm + damping * damping * BLOCK)
    a = scaling * inverse
    b = scaling * damping
    r_g, r_p, r_i = a * (10.0 - 2.0 * b) / 16.0, a * a / 16.0, b * (10.0 - b) / 16.0
    w_g, w_p, w_i = a * (5.0 - 2.0 * b) / 4.0, a * a / 4.0, b * (5.0 - b) / 4.0
    for part in range(BLOCK // STEP):
        here = slice(part * STEP, (part + 1) * STEP)
        product = jnp.dot(g_ref[here, :], g_ref[...], preferred_element_type=F32)
        value = g_ref[here, :].astype(F32)
        on = diagonal(part * STEP, STEP)
        rb_ref[here, :] = (r_g * value - r_p * product + jnp.where(on, r_i, 0.0)).astype(BF16)
        inner = w_g * value - w_p * product + jnp.where(on, w_i, 0.0)
        w_ref[here, :] = inner
        wb_ref[here, :] = inner.astype(BF16)
    for part in range(BLOCK // STEP):
        here = slice(part * STEP, (part + 1) * STEP)
        product = jnp.dot(rb_ref[here, :], wb_ref[...], preferred_element_type=F32)
        inner = (25.0 / 16.0) * w_ref[here, :] - product
        v_ref[here, :] = inner
        vb_ref[here, :] = inner.astype(BF16)
    quarter = jnp.sqrt(jnp.sqrt(scaling)) * 0.25
    for part in range(BLOCK // STEP):
        here = slice(part * STEP, (part + 1) * STEP)
        product = jnp.dot(rb_ref[here, :], vb_ref[...], preferred_element_type=F32)
        inner = product - (25.0 / 16.0) * v_ref[here, :]
        on = diagonal(part * STEP, STEP)
        inner = inner - (1.25 * a) * g_ref[here, :].astype(F32)
        inner = inner + jnp.where(on, 6.25 - 1.25 * b, 0.0)
        root[here, :] = (quarter * inner).astype(BF16)

    if side == 0:
        return
    index = (place[Z] * SIDE + place[X]) * 2
    for target, who in ((root_own, place[CORE]), (root_other, 1 - place[CORE])):
        target[...] = jnp.zeros_like(target)
        for block, source in enumerate((before, root)):

            @pl.when(owners[place[CORE], place[TP] * 2 + block] == index + who)
            def _():
                target[...] = source[...]


def update_other_kernel(place, counts, other, root_zero, root_one, update):
    _, value = masked_rows(place, counts, other[...], other[...])
    for block, root in enumerate((root_zero, root_one)):
        columns = slice(block * BLOCK, (block + 1) * BLOCK)
        product = jnp.dot(value[:, columns], root[...], preferred_element_type=F32)
        update[:, columns] = product.astype(BF16)


def update_own_kernel(place, counts, own, root_zero, root_one, update):
    value, _ = masked_rows(place, counts, own[0], own[0])
    for block, root in enumerate((root_zero, root_one)):

        @pl.when(pl.program_id(0) == block)
        def _():
            update[0] = jnp.dot(value, root[...], preferred_element_type=F32).astype(BF16)


def finish_kernel(place, _, back, root_own, root_back, update, owned):
    update[0] = back[...]
    owned[...] = root_own[...] + root_back[...]


def shifted(value, axis, distance):
    return lax.ppermute(value, axis, [(k, (k + distance) % SIDE) for k in range(SIDE)])


def swapped(value):
    return lax.ppermute(value, "core", [(0, 1), (1, 0)])


def resident(value):
    return pltpu.with_memory_space_constraint(value, pltpu.VMEM)


def local_call(kernel, name, ins, outs):
    return pl.pallas_call(
        kernel,
        in_specs=[RESIDENT] * len(ins),
        out_specs=[RESIDENT] * len(outs),
        out_shape=[pltpu.VMEM(*each) for each in outs],
        compiler_params=params(4),
        name=name,
    )(*[resident(value) for value in ins])


ORDER = (2, 1, 3)


def body(gradients, row_counts, block_owner):
    core = lax.axis_index("core")
    place = jnp.stack([lax.axis_index(name) for name in ("z", "x", "core", "tp")])
    place = place.astype(jnp.int32)
    _, row_slots, columns = gradients.shape
    square = (BLOCK, BLOCK)
    part = (row_slots, BLOCK)

    away = lax.dynamic_index_in_dim(gradients, 1 - core, 0, keepdims=False)
    other = resident(swapped(away))

    def packed_gram(side):
        return pl.pallas_call(
            functools.partial(gram_kernel, side),
            grid_spec=pltpu.PrefetchScalarGridSpec(
                num_scalar_prefetch=2,
                grid=(1,),
                in_specs=[
                    pl.BlockSpec((1,) + part, lambda i, p, c: (p[CORE], 0, side)),
                    RESIDENT,
                ],
                out_specs=[RESIDENT] * 4,
                scratch_shapes=[
                    pltpu.VMEM((2 * row_slots, BLOCK + BLOCK // 2), BF16),
                    pltpu.VMEM((16, HALF, WIDE), F32),
                ],
            ),
            out_shape=[pltpu.VMEM(LINE, BF16 if k else F32) for k in range(SIDE)],
            compiler_params=params(16),
            name=f"gram_{side}",
        )(place, row_counts, gradients, other)

    def exchange(values, axis, sign):
        received = list(values)
        for k in ORDER:
            received[k] = shifted(values[k], axis, sign * k)
        return received

    outer = ("x", "z")
    inner = ("z", "x")
    chunks = [(CHUNK, BF16 if k else F32) for k in range(SIDE)]
    both = range(2)
    held = [packed_gram(side) for side in both]
    held = [exchange(held[side], outer[side], 1) for side in both]
    held = [local_call(first_sum_kernel, f"first_{side}", held[side], chunks) for side in both]
    held = [exchange(held[side], inner[side], 1) for side in both]
    held = [
        local_call(second_sum_kernel, f"second_{side}", held[side], [(CHUNK, BF16)])
        for side in both
    ]
    held = [exchange(held[side] * SIDE, inner[side], -1) for side in both]
    held = [local_call(line_kernel, f"line_{side}", held[side], [(LINE, BF16)]) for side in both]
    held = [exchange(held[side] * SIDE, outer[side], -1) for side in both]

    def root_of(side, ins, outs):
        return pl.pallas_call(
            functools.partial(root_kernel, side),
            grid_spec=pltpu.PrefetchScalarGridSpec(
                num_scalar_prefetch=3,
                grid=(1,),
                in_specs=[RESIDENT] * len(ins),
                out_specs=[RESIDENT] * outs,
                scratch_shapes=[
                    pltpu.VMEM(square, BF16),
                    pltpu.VMEM(square, F32),
                    pltpu.VMEM(square, F32),
                    pltpu.VMEM(square, BF16),
                    pltpu.VMEM(square, BF16),
                    pltpu.VMEM(square, BF16),
                ],
            ),
            out_shape=[pltpu.VMEM(square, BF16)] * outs,
            compiler_params=params(30),
            name=f"root_{side}",
        )(place, row_counts, block_owner, *[resident(value) for value in ins])

    root_zero = resident(root_of(0, held[0], 1)[0])
    root_one, root_own, root_other = root_of(1, held[1] + [root_zero], 3)
    root_back = resident(swapped(root_other))
    roots = (root_zero, resident(root_one))

    update_other = pl.pallas_call(
        update_other_kernel,
        grid_spec=pltpu.PrefetchScalarGridSpec(
            num_scalar_prefetch=2,
            grid=(1,),
            in_specs=[RESIDENT] * 3,
            out_specs=RESIDENT,
        ),
        out_shape=pltpu.VMEM((row_slots, columns), BF16),
        compiler_params=params(16),
        name="update_other",
    )(place, row_counts, other, *roots)
    update_back = resident(swapped(update_other))
    update = pl.pallas_call(
        update_own_kernel,
        grid_spec=pltpu.PrefetchScalarGridSpec(
            num_scalar_prefetch=2,
            grid=(2,),
            in_specs=[
                pl.BlockSpec((1,) + part, lambda k, p, c: (p[CORE], 0, k)),
                RESIDENT,
                RESIDENT,
            ],
            out_specs=pl.BlockSpec((1,) + part, lambda k, p, c: (p[CORE], 0, k)),
        ),
        out_shape=jax.ShapeDtypeStruct(gradients.shape, BF16),
        compiler_params=params(16),
        name="update_own",
    )(place, row_counts, gradients, *roots)

    steps = 2
    strip = (BLOCK // steps, BLOCK)
    band = (row_slots // steps, columns)
    return pl.pallas_call(
        finish_kernel,
        grid_spec=pltpu.PrefetchScalarGridSpec(
            num_scalar_prefetch=1,
            grid=(steps,),
            in_specs=[
                pl.BlockSpec(memory_space=pl.ANY),
                pl.BlockSpec(band, lambda k, p: (k, 0)),
                pl.BlockSpec(strip, lambda k, p: (k, 0)),
                pl.BlockSpec(strip, lambda k, p: (k, 0)),
            ],
            out_specs=[
                pl.BlockSpec((1,) + band, lambda k, p: (1 - p[CORE], k, 0)),
                pl.BlockSpec(strip, lambda k, p: (k, 0)),
            ],
        ),
        out_shape=[
            jax.ShapeDtypeStruct(gradients.shape, BF16),
            jax.ShapeDtypeStruct(square, BF16),
        ],
        input_output_aliases={1: 0},
        compiler_params=params(16),
        name="finish",
    )(place, update, update_back, resident(root_own), root_back)


def solution(mesh):
    cores = Mesh(mesh.devices.reshape(SIDE, SIDE, 2, SIDE), ("z", "x", "core", "tp"))
    rows = ("z", "x", "core")
    return jax.shard_map(
        body,
        mesh=cores,
        in_specs=(P(None, rows, "tp"), P(), P()),
        out_specs=(P(None, rows, "tp"), P(rows, "tp")),
        check_vma=False,
    )
```

```python
import functools

import jax
import jax.numpy as jnp
from jax import lax
from jax.experimental import pallas as pl
from jax.experimental.pallas import tpu as pltpu
from jax.sharding import Mesh, PartitionSpec as P


BLOCK = 1024
TILE = 128
HALF = 64
WIDE = 640
SIDE = 4
LAYERS = 2
STEP = 512
damping = 0.01
F32 = jnp.float32
BF16 = jnp.bfloat16


def params(mebibytes):
    return pltpu.CompilerParams(vmem_limit_bytes=mebibytes * 1024 * 1024)


RESIDENT = pl.BlockSpec(memory_space=pltpu.VMEM)
LINE = (SIDE, HALF, WIDE)
Z, X, CORE, TP = range(4)
OUT = (0, 2, 1, 3)
BACK = (0, 1, 3, 2)
ROWS = ("z", "x", "core")


def valid_rows(place, counts, who, value):
    rows = lax.broadcasted_iota(jnp.int32, value.shape, 0)
    limit = counts[(place[Z] * SIDE + place[X]) * 2 + who]
    return jnp.where(rows < limit, value, jnp.zeros_like(value))


def chunk_of(place, first, second):
    z = second + place[CORE] * (first - second)
    x = first + place[CORE] * (second - first)
    return ((place[Z] + z) % SIDE) * SIDE + (place[X] + x) % SIDE


def away_kernel(place, half, out):
    out[pl.program_id(0)] = half[0]


def gram_kernel(place, counts, own, other, *refs):
    outs, (wide, gram) = refs[:SIDE], refs[SIDE:]
    rows = own.shape[1]
    wide[:rows, :BLOCK] = valid_rows(place, counts, place[CORE], own[0])
    wide[rows:, :BLOCK] = valid_rows(place, counts, 1 - place[CORE], other[0])
    wide[:, BLOCK:] = wide[:, : BLOCK // 2]
    for pair in range(4):
        start = pair * 2 * TILE
        part = lax.dot_general(
            wide[:, start : start + 2 * TILE],
            wide[:, start : start + 6 * TILE],
            (((0,), (0,)), ((), ())),
            preferred_element_type=F32,
        )
        for quarter in range(4):
            shift = TILE * (quarter // 2)
            gram[4 * pair + quarter] = part[
                quarter * HALF : (quarter + 1) * HALF, shift : shift + WIDE
            ]
    for first in range(SIDE):
        for second in range(SIDE):
            value = gram[chunk_of(place, first, second)]
            outs[first][second] = value.astype(outs[first].dtype)


def first_sum_kernel(*refs):
    for second in range(SIDE):
        value = refs[0][second]
        for k in range(1, SIDE):
            value = value + refs[k][second].astype(F32)
        refs[SIDE][second] = value.astype(BF16)


def second_sum_kernel(*refs):
    for second in range(SIDE):
        value = refs[0][second].astype(F32)
        for slot in range(1, SIDE):
            k = BACK[slot]
            value = value + refs[slot][(second + k) % SIDE].astype(F32)
        refs[SIDE][second] = value.astype(BF16)


def diagonal(start, rows):
    row = lax.broadcasted_iota(jnp.int32, (rows, BLOCK), 0) + start
    return row == lax.broadcasted_iota(jnp.int32, (rows, BLOCK), 1)


def root_kernel(layer, place, counts, owners, *refs):
    sets, refs = refs[:4], refs[4:]
    if layer == 1:
        before, refs = refs[0], refs[1:]
    root, refs = refs[0], refs[1:]
    if layer == 1:
        (root_own, root_other), refs = refs[:2], refs[2:]
    g_ref, w_ref, v_ref, rb_ref, wb_ref, vb_ref = refs

    for slot, first in enumerate(BACK):
        for second in range(SIDE):
            chunk = chunk_of(place, first, second)
            row = pl.multiple_of(chunk * HALF, HALF)
            value = sets[slot][second]
            for k in range(WIDE // TILE):
                column = pl.multiple_of(((chunk // 2 + k) % 8) * TILE, TILE)
                g_ref[pl.ds(row, HALF), pl.ds(column, TILE)] = value[:, k * TILE : (k + 1) * TILE]

    for slab in range(8):
        for k in range(1, 4):
            far = (slab + k) % 8
            here = slice(slab * TILE, (slab + 1) * TILE)
            there = slice(far * TILE, (far + 1) * TILE)
            g_ref[there, here] = g_ref[here, there].T

    squares = jnp.zeros((1, BLOCK), F32)
    trace = jnp.zeros((1, TILE), F32)
    row = lax.broadcasted_iota(jnp.int32, (TILE, TILE), 0)
    corner = row == lax.broadcasted_iota(jnp.int32, (TILE, TILE), 1)
    for slab in range(8):
        here = slice(slab * TILE, (slab + 1) * TILE)
        value = g_ref[here, :].astype(F32)
        squares = squares + jnp.sum(value * value, axis=0, keepdims=True)
        value = jnp.where(corner, g_ref[here, here].astype(F32), 0.0)
        trace = trace + jnp.sum(value, axis=0, keepdims=True)
    squares = jnp.sum(squares, axis=1, keepdims=True)
    trace = jnp.sum(trace, axis=1, keepdims=True)
    total = counts[0]
    for k in range(1, counts.shape[0]):
        total = total + counts[k]
    inverse = 1.0 / jnp.full((1, 1), total, jnp.int32).astype(F32)
    norm = squares * inverse * inverse + 2.0 * damping * inverse * trace
    scaling = 2.5 / jnp.sqrt(norm + damping * damping * BLOCK)
    a = scaling * inverse
    b = scaling * damping
    r_g, r_p, r_i = a * (10.0 - 2.0 * b) / 16.0, a * a / 16.0, b * (10.0 - b) / 16.0
    w_g, w_p, w_i = a * (5.0 - 2.0 * b) / 4.0, a * a / 4.0, b * (5.0 - b) / 4.0
    for part in range(BLOCK // STEP):
        here = slice(part * STEP, (part + 1) * STEP)
        product = jnp.dot(g_ref[here, :], g_ref[...], preferred_element_type=F32)
        value = g_ref[here, :].astype(F32)
        on = diagonal(part * STEP, STEP)
        rb_ref[here, :] = (r_g * value - r_p * product + jnp.where(on, r_i, 0.0)).astype(BF16)
        inner = w_g * value - w_p * product + jnp.where(on, w_i, 0.0)
        w_ref[here, :] = inner
        wb_ref[here, :] = inner.astype(BF16)
    for part in range(BLOCK // STEP):
        here = slice(part * STEP, (part + 1) * STEP)
        product = jnp.dot(rb_ref[here, :], wb_ref[...], preferred_element_type=F32)
        inner = (25.0 / 16.0) * w_ref[here, :] - product
        v_ref[here, :] = inner
        vb_ref[here, :] = inner.astype(BF16)
    quarter = jnp.sqrt(jnp.sqrt(scaling)) * 0.25
    for part in range(BLOCK // STEP):
        here = slice(part * STEP, (part + 1) * STEP)
        product = jnp.dot(rb_ref[here, :], vb_ref[...], preferred_element_type=F32)
        inner = product - (25.0 / 16.0) * v_ref[here, :]
        on = diagonal(part * STEP, STEP)
        inner = inner - (1.25 * a) * g_ref[here, :].astype(F32)
        inner = inner + jnp.where(on, 6.25 - 1.25 * b, 0.0)
        root[here, :] = (quarter * inner).astype(BF16)

    if layer == 0:
        return
    index = (place[Z] * SIDE + place[X]) * 2
    for target, who in ((root_own, place[CORE]), (root_other, 1 - place[CORE])):
        target[...] = jnp.zeros_like(target)
        for k, source in enumerate((before, root)):

            @pl.when(owners[k, place[TP] * 2 + place[CORE]] == index + who)
            def _():
                target[...] = source[...]


def update_kernel(other_core, place, counts, rows, root_zero, root_one, update):
    who = 1 - place[CORE] if other_core else place[CORE]
    for layer, root in enumerate((root_zero, root_one)):
        value = valid_rows(place, counts, who, rows[layer])
        product = jnp.dot(value, root[...], preferred_element_type=F32)
        update[layer] = product.astype(BF16)


def finish_kernel(place, owners, own, back, root_own, root_back, update, owned, sems):
    core = place[CORE]
    here = pl.ds(pl.multiple_of(core * BLOCK, BLOCK), BLOCK)
    there = pl.ds(pl.multiple_of((1 - core) * BLOCK, BLOCK), BLOCK)
    copies = [
        pltpu.make_async_copy(own, update.at[:, :, here], sems.at[0]),
        pltpu.make_async_copy(back, update.at[:, :, there], sems.at[1]),
    ]
    for copy in copies:
        copy.start()
    index = (place[Z] * SIDE + place[X]) * 2 + core
    column = place[TP] * 2 + core
    mine = jnp.logical_or(owners[0, column] == index, owners[1, column] == index)

    @pl.when(mine)
    def _():
        copy = pltpu.make_async_copy(root_own, owned, sems.at[2])
        copy.start()
        copy.wait()

    @pl.when(jnp.logical_not(mine))
    def _():
        copy = pltpu.make_async_copy(root_back, owned, sems.at[3])
        copy.start()
        copy.wait()

    for copy in copies:
        copy.wait()


def shifted(value, outer, distance):
    pairs = []
    for z in range(SIDE):
        for x in range(SIDE):
            for core in range(2):
                if outer == (core == 0):
                    there = (z, (x + distance) % SIDE)
                else:
                    there = ((z + distance) % SIDE, x)
                pairs.append(
                    ((z * SIDE + x) * 2 + core, (there[0] * SIDE + there[1]) * 2 + core)
                )
    return lax.ppermute(value, ROWS, pairs)


def swapped(value):
    return lax.ppermute(value, "core", [(0, 1), (1, 0)])


def resident(value):
    return pltpu.with_memory_space_constraint(value, pltpu.VMEM)


def local_call(kernel, name, ins, outs):
    return pl.pallas_call(
        kernel,
        in_specs=[RESIDENT] * len(ins),
        out_specs=[RESIDENT] * len(outs),
        out_shape=[pltpu.VMEM(*each) for each in outs],
        compiler_params=params(4),
        name=name,
    )(*[resident(value) for value in ins])


def body(gradients, row_counts, block_owner):
    place = jnp.stack([lax.axis_index(name) for name in ("z", "x", "core", "tp")])
    place = place.astype(jnp.int32)
    _, row_slots, _ = gradients.shape
    square = (BLOCK, BLOCK)
    part = (row_slots, BLOCK)
    parts = (LAYERS,) + part

    away = pl.pallas_call(
        away_kernel,
        grid_spec=pltpu.PrefetchScalarGridSpec(
            num_scalar_prefetch=1,
            grid=(LAYERS,),
            in_specs=[pl.BlockSpec((1,) + part, lambda k, p: (k, 0, 1 - p[CORE]))],
            out_specs=RESIDENT,
        ),
        out_shape=pltpu.VMEM(parts, BF16),
        compiler_params=params(8),
        name="away",
    )(place, pltpu.with_memory_space_constraint(gradients, pltpu.HBM))
    other = resident(swapped(away))

    def gram_of(layer):
        return pl.pallas_call(
            gram_kernel,
            grid_spec=pltpu.PrefetchScalarGridSpec(
                num_scalar_prefetch=2,
                grid=(1,),
                in_specs=[
                    pl.BlockSpec((1,) + part, lambda i, p, c: (layer, 0, p[CORE])),
                    pl.BlockSpec((1,) + part, lambda i, p, c: (layer, 0, 0)),
                ],
                out_specs=[RESIDENT] * SIDE,
                scratch_shapes=[
                    pltpu.VMEM((2 * row_slots, BLOCK + BLOCK // 2), BF16),
                    pltpu.VMEM((16, HALF, WIDE), F32),
                ],
            ),
            out_shape=[pltpu.VMEM(LINE, BF16 if k else F32) for k in range(SIDE)],
            compiler_params=params(16),
            name=f"gram_{layer}",
        )(place, row_counts, gradients, other)

    def exchange(values, outer, sign, order):
        return [values[0]] + [shifted(values[k], outer, sign * k) for k in order[1:]]

    sets = []
    for layer in range(LAYERS):
        grams = exchange(gram_of(layer), True, 1, OUT)
        (line,) = local_call(first_sum_kernel, f"first_{layer}", grams, [(LINE, BF16)])
        lines = exchange([line] * SIDE, False, 1, BACK)
        (line,) = local_call(second_sum_kernel, f"second_{layer}", lines, [(LINE, BF16)])
        sets.append(exchange([line] * SIDE, True, -1, BACK))

    def root_of(layer, ins, outs):
        return pl.pallas_call(
            functools.partial(root_kernel, layer),
            grid_spec=pltpu.PrefetchScalarGridSpec(
                num_scalar_prefetch=3,
                grid=(1,),
                in_specs=[RESIDENT] * len(ins),
                out_specs=[RESIDENT] * outs,
                scratch_shapes=[
                    pltpu.VMEM(square, BF16),
                    pltpu.VMEM(square, F32),
                    pltpu.VMEM(square, F32),
                    pltpu.VMEM(square, BF16),
                    pltpu.VMEM(square, BF16),
                    pltpu.VMEM(square, BF16),
                ],
            ),
            out_shape=[pltpu.VMEM(square, BF16)] * outs,
            compiler_params=params(30),
            name=f"root_{layer}",
        )(place, row_counts, block_owner, *[resident(value) for value in ins])

    root_zero = resident(root_of(0, sets[0], 1)[0])
    root_one, root_own, root_other = root_of(1, sets[1] + [root_zero], 3)
    root_back = resident(swapped(root_other))
    roots = (root_zero, resident(root_one))

    def update_of(other_core, rows, spec, name):
        return pl.pallas_call(
            functools.partial(update_kernel, other_core),
            grid_spec=pltpu.PrefetchScalarGridSpec(
                num_scalar_prefetch=2,
                grid=(1,),
                in_specs=[spec, RESIDENT, RESIDENT],
                out_specs=RESIDENT,
            ),
            out_shape=pltpu.VMEM(parts, BF16),
            compiler_params=params(16),
            name=name,
        )(place, row_counts, rows, *roots)

    update_back = resident(swapped(update_of(True, other, RESIDENT, "update_other")))
    own_columns = pl.BlockSpec(parts, lambda i, p, c: (0, 0, p[CORE]))
    update_own = resident(update_of(False, gradients, own_columns, "update_own"))
    anywhere = pl.BlockSpec(memory_space=pl.ANY)
    return pl.pallas_call(
        finish_kernel,
        grid_spec=pltpu.PrefetchScalarGridSpec(
            num_scalar_prefetch=2,
            grid=(1,),
            in_specs=[RESIDENT] * 4,
            out_specs=[anywhere, anywhere],
            scratch_shapes=[pltpu.SemaphoreType.DMA((4,))],
        ),
        out_shape=[
            jax.ShapeDtypeStruct(gradients.shape, BF16),
            jax.ShapeDtypeStruct(square, BF16),
        ],
        compiler_params=params(4),
        name="finish",
    )(place, block_owner, update_own, update_back, resident(root_own), root_back)


def solution(mesh):
    cores = Mesh(mesh.devices.reshape(SIDE, SIDE, 2, SIDE), ROWS + ("tp",))
    return jax.shard_map(
        body,
        mesh=cores,
        in_specs=(P(None, ROWS, "tp"), P(), P()),
        out_specs=(P(None, ROWS, "tp"), P(ROWS, "tp")),
        check_vma=False,
    )
```

```python
import functools

import jax
import jax.numpy as jnp
from jax import lax
from jax.experimental import pallas as pl
from jax.experimental.pallas import tpu as pltpu
from jax.sharding import Mesh, PartitionSpec as P


BLOCK = 1024
TILE = 128
HALF = 64
WIDE = 640
SIDE = 4
LAYERS = 2
STEP = 512
damping = 0.01
F32 = jnp.float32
BF16 = jnp.bfloat16


def params(mebibytes):
    return pltpu.CompilerParams(vmem_limit_bytes=mebibytes * 1024 * 1024)


def products(count):
    return pl.CostEstimate(flops=2 * count, transcendentals=0, bytes_accessed=0)


RESIDENT = pl.BlockSpec(memory_space=pltpu.VMEM)
LINE = (SIDE, HALF, WIDE)
PAIR = (LAYERS, HALF, WIDE)
Z, X, CORE, TP = range(4)
OUT = (0, 1, 3, 2)
BACK = (0, 1, 3, 2)
ROWS = ("z", "x", "core")


def valid_rows(place, counts, who, value):
    rows = lax.broadcasted_iota(jnp.int32, value.shape, 0)
    limit = counts[(place[Z] * SIDE + place[X]) * 2 + who]
    return jnp.where(rows < limit, value, jnp.zeros_like(value))


def chunk_of(place, first, second):
    z = second + place[CORE] * (first - second)
    x = first + place[CORE] * (second - first)
    return ((place[Z] + z) % SIDE) * SIDE + (place[X] + x) % SIDE


def away_kernel(place, gradients, out, sem):
    columns = pl.ds(pl.multiple_of((1 - place[CORE]) * BLOCK, BLOCK), BLOCK)
    copy = pltpu.make_async_copy(gradients.at[:, :, columns], out, sem)
    copy.start()
    copy.wait()


def gram_kernel(place, counts, own, other, *refs):
    outs, (wide, gram) = refs[:SIDE], refs[SIDE:]
    rows = own.shape[1]
    for layer in range(LAYERS):
        wide[:rows, :BLOCK] = valid_rows(place, counts, place[CORE], own[layer])
        wide[rows:, :BLOCK] = valid_rows(place, counts, 1 - place[CORE], other[layer])
        wide[:, BLOCK:] = wide[:, : BLOCK // 2]
        for pair in range(4):
            start = pair * 2 * TILE
            part = lax.dot_general(
                wide[:, start : start + 2 * TILE],
                wide[:, start : start + 6 * TILE],
                (((0,), (0,)), ((), ())),
                preferred_element_type=F32,
            )
            for quarter in range(4):
                shift = TILE * (quarter // 2)
                gram[4 * pair + quarter] = part[
                    quarter * HALF : (quarter + 1) * HALF, shift : shift + WIDE
                ]
        for first in range(SIDE):
            for second in range(SIDE):
                value = gram[chunk_of(place, first, second)]
                outs[first][layer, second] = value.astype(outs[first].dtype)


def first_sum_kernel(*refs):
    ins, outs = refs[:SIDE], refs[SIDE:]
    for layer in range(LAYERS):
        for second in range(SIDE):
            value = ins[0][layer, second]
            for k in range(1, SIDE):
                value = value + ins[k][layer, second].astype(F32)
            outs[second][layer] = value.astype(outs[second].dtype)


def second_sum_kernel(*refs):
    value = refs[0][...]
    for k in range(1, SIDE):
        value = value + refs[k][...].astype(F32)
    refs[SIDE][...] = value.astype(BF16)


def line_kernel(*refs):
    for layer in range(LAYERS):
        for k in range(SIDE):
            refs[SIDE + layer][BACK[k]] = refs[k][layer]


def diagonal(start, rows):
    row = lax.broadcasted_iota(jnp.int32, (rows, BLOCK), 0) + start
    return row == lax.broadcasted_iota(jnp.int32, (rows, BLOCK), 1)


def root_kernel(layer, place, counts, owners, *refs):
    sets, refs = refs[:SIDE], refs[SIDE:]
    if layer == 1:
        before, root, root_own, root_other, factors, g_ref, v_ref, rb_ref, vb_ref = refs[:9]
        w_ref, wb_ref = refs[9:]
    else:
        root, g_ref, w_ref, v_ref, rb_ref, wb_ref, vb_ref = refs

    for slot, first in enumerate(BACK):
        for second in range(SIDE):
            chunk = chunk_of(place, first, second)
            row = pl.multiple_of(chunk * HALF, HALF)
            value = sets[slot][second]
            for k in range(WIDE // TILE):
                column = pl.multiple_of(((chunk // 2 + k) % 8) * TILE, TILE)
                g_ref[pl.ds(row, HALF), pl.ds(column, TILE)] = value[:, k * TILE : (k + 1) * TILE]

    for slab in range(8):
        for k in range(1, 4):
            far = (slab + k) % 8
            here = slice(slab * TILE, (slab + 1) * TILE)
            there = slice(far * TILE, (far + 1) * TILE)
            g_ref[there, here] = g_ref[here, there].T

    squares = jnp.zeros((1, BLOCK), F32)
    trace = jnp.zeros((1, TILE), F32)
    row = lax.broadcasted_iota(jnp.int32, (TILE, TILE), 0)
    corner = row == lax.broadcasted_iota(jnp.int32, (TILE, TILE), 1)
    for slab in range(8):
        here = slice(slab * TILE, (slab + 1) * TILE)
        value = g_ref[here, :].astype(F32)
        squares = squares + jnp.sum(value * value, axis=0, keepdims=True)
        value = jnp.where(corner, g_ref[here, here].astype(F32), 0.0)
        trace = trace + jnp.sum(value, axis=0, keepdims=True)
    squares = jnp.sum(squares, axis=1, keepdims=True)
    trace = jnp.sum(trace, axis=1, keepdims=True)
    total = counts[0]
    for k in range(1, counts.shape[0]):
        total = total + counts[k]
    inverse = 1.0 / jnp.full((1, 1), total, jnp.int32).astype(F32)
    norm = squares * inverse * inverse + 2.0 * damping * inverse * trace
    scaling = 2.5 / jnp.sqrt(norm + damping * damping * BLOCK)
    a = scaling * inverse
    b = scaling * damping
    r_g, r_p, r_i = a * (10.0 - 2.0 * b) / 16.0, a * a / 16.0, b * (10.0 - b) / 16.0
    w_g, w_p, w_i = a * (5.0 - 2.0 * b) / 4.0, a * a / 4.0, b * (5.0 - b) / 4.0
    for part in range(BLOCK // STEP):
        here = slice(part * STEP, (part + 1) * STEP)
        product = jnp.dot(g_ref[here, :], g_ref[...], preferred_element_type=F32)
        value = g_ref[here, :].astype(F32)
        on = diagonal(part * STEP, STEP)
        rb_ref[here, :] = (r_g * value - r_p * product + jnp.where(on, r_i, 0.0)).astype(BF16)
        inner = w_g * value - w_p * product + jnp.where(on, w_i, 0.0)
        w_ref[here, :] = inner
        wb_ref[here, :] = inner.astype(BF16)
    for part in range(BLOCK // STEP):
        here = slice(part * STEP, (part + 1) * STEP)
        product = jnp.dot(rb_ref[here, :], wb_ref[...], preferred_element_type=F32)
        inner = (25.0 / 16.0) * w_ref[here, :] - product
        v_ref[here, :] = inner
        vb_ref[here, :] = inner.astype(BF16)
    quarter = jnp.sqrt(jnp.sqrt(scaling)) * 0.25
    halves = 1 if layer == 1 else 2
    for part in range(halves):
        here = slice(part * STEP, (part + 1) * STEP)
        root[here, :] = root_rows(part * STEP, g_ref, v_ref, rb_ref, vb_ref, quarter, a, b)
    if layer == 1:
        for k, value in enumerate((quarter, a, b)):
            factors[k : k + 1, :] = jnp.broadcast_to(value, (1, TILE))
        pick_owned(place, owners, before[:STEP, :], root, root_own, root_other)


def root_rows(start, g_ref, v_ref, rb_ref, vb_ref, quarter, a, b):
    here = slice(start, start + STEP)
    product = jnp.dot(rb_ref[here, :], vb_ref[...], preferred_element_type=F32)
    inner = product - (25.0 / 16.0) * v_ref[here, :]
    inner = inner - (1.25 * a) * g_ref[here, :].astype(F32)
    inner = inner + jnp.where(diagonal(start, STEP), 6.25 - 1.25 * b, 0.0)
    return (quarter * inner).astype(BF16)


def pick_owned(place, owners, zero, one, root_own, root_other):
    index = (place[Z] * SIDE + place[X]) * 2
    for target, who in ((root_own, place[CORE]), (root_other, 1 - place[CORE])):
        target[...] = jnp.zeros_like(target)
        for k, source in enumerate((zero, one)):

            @pl.when(owners[k, place[TP] * 2 + place[CORE]] == index + who)
            def _():
                target[...] = source[...]


def lower_kernel(place, owners, before, factors, g_ref, v_ref, rb_ref, vb_ref, *refs):
    root, root_own, root_other = refs
    quarter, a, b = (factors[k : k + 1, :1] for k in range(3))
    root[...] = root_rows(STEP, g_ref, v_ref, rb_ref, vb_ref, quarter, a, b)
    pick_owned(place, owners, before[STEP:, :], root, root_own, root_other)


def update_kernel(other_core, place, counts, rows, zero, upper, lower, update):
    who = 1 - place[CORE] if other_core else place[CORE]
    value = valid_rows(place, counts, who, rows[0])
    update[0] = jnp.dot(value, zero[...], preferred_element_type=F32).astype(BF16)
    value = valid_rows(place, counts, who, rows[1])
    product = jnp.dot(value[:, :STEP], upper[...], preferred_element_type=F32)
    product = product + jnp.dot(value[:, STEP:], lower[...], preferred_element_type=F32)
    update[1] = product.astype(BF16)


def finish_kernel(place, owners, own, back, *refs):
    mine, theirs, (update, owned, sems) = refs[:2], refs[2:4], refs[4:]
    core = place[CORE]
    here = pl.ds(pl.multiple_of(core * BLOCK, BLOCK), BLOCK)
    there = pl.ds(pl.multiple_of((1 - core) * BLOCK, BLOCK), BLOCK)
    copies = [
        pltpu.make_async_copy(own, update.at[:, :, here], sems.at[0]),
        pltpu.make_async_copy(back, update.at[:, :, there], sems.at[1]),
    ]
    for copy in copies:
        copy.start()
    index = (place[Z] * SIDE + place[X]) * 2 + core
    column = place[TP] * 2 + core
    is_mine = jnp.logical_or(owners[0, column] == index, owners[1, column] == index)

    def write(sources, first):
        parts = [
            pltpu.make_async_copy(source, owned.at[pl.ds(k * STEP, STEP)], sems.at[first + k])
            for k, source in enumerate(sources)
        ]
        for copy in parts:
            copy.start()
        for copy in parts:
            copy.wait()

    @pl.when(is_mine)
    def _():
        write(mine, 2)

    @pl.when(jnp.logical_not(is_mine))
    def _():
        write(theirs, 4)

    for copy in copies:
        copy.wait()


def shifted(value, outer, distance):
    pairs = []
    for z in range(SIDE):
        for x in range(SIDE):
            for core in range(2):
                if outer == (core == 0):
                    there = (z, (x + distance) % SIDE)
                else:
                    there = ((z + distance) % SIDE, x)
                pairs.append(
                    ((z * SIDE + x) * 2 + core, (there[0] * SIDE + there[1]) * 2 + core)
                )
    return lax.ppermute(value, ROWS, pairs)


def swapped(value):
    return lax.ppermute(value, "core", [(0, 1), (1, 0)])


def resident(value):
    return pltpu.with_memory_space_constraint(value, pltpu.VMEM)


def local_call(kernel, ins, outs):
    return pl.pallas_call(
        kernel,
        in_specs=[RESIDENT] * len(ins),
        out_specs=[RESIDENT] * len(outs),
        out_shape=[pltpu.VMEM(*each) for each in outs],
        compiler_params=params(4),
    )(*[resident(value) for value in ins])


def body(gradients, row_counts, block_owner):
    place = jnp.stack([lax.axis_index(name) for name in ("z", "x", "core", "tp")])
    place = place.astype(jnp.int32)
    _, row_slots, columns = gradients.shape
    square = (BLOCK, BLOCK)
    part = (row_slots, BLOCK)
    parts = (LAYERS,) + part

    away = pl.pallas_call(
        away_kernel,
        grid_spec=pltpu.PrefetchScalarGridSpec(
            num_scalar_prefetch=1,
            grid=(1,),
            in_specs=[pl.BlockSpec(memory_space=pl.ANY)],
            out_specs=RESIDENT,
            scratch_shapes=[pltpu.SemaphoreType.DMA],
        ),
        out_shape=pltpu.VMEM(parts, BF16),
        compiler_params=params(4),
        name="away",
    )(place, pltpu.with_memory_space_constraint(gradients, pltpu.HBM))
    other = resident(swapped(away))

    grams = pl.pallas_call(
        gram_kernel,
        grid_spec=pltpu.PrefetchScalarGridSpec(
            num_scalar_prefetch=2,
            grid=(1,),
            in_specs=[pl.BlockSpec(parts, lambda i, p, c: (0, 0, p[CORE])), RESIDENT],
            out_specs=[RESIDENT] * SIDE,
            scratch_shapes=[
                pltpu.VMEM((2 * row_slots, BLOCK + BLOCK // 2), BF16),
                pltpu.VMEM((16, HALF, WIDE), F32),
            ],
        ),
        out_shape=[pltpu.VMEM((LAYERS,) + LINE, BF16 if k else F32) for k in range(SIDE)],
        compiler_params=params(20),
        name="gram",
    )(place, row_counts, gradients, other)

    def exchange(values, outer, sign):
        return [values[0]] + [shifted(values[k], outer, sign * k) for k in (OUT if sign > 0 else BACK)[1:]]

    outs = [(PAIR, BF16 if k else F32) for k in range(SIDE)]
    summed = local_call(first_sum_kernel, exchange(grams, True, 1), outs)
    summed = exchange(summed, False, 1)
    (reduced,) = local_call(second_sum_kernel, summed, [(PAIR, BF16)])
    pieces = exchange([reduced] * SIDE, False, -1)
    lines = local_call(line_kernel, pieces, [(LINE, BF16)] * LAYERS)
    sets = [exchange([line] * SIDE, True, -1) for line in lines]

    strip = (STEP, BLOCK)
    scratch = [(square, BF16), (square, F32), (square, F32)] + [(square, BF16)] * 3

    def root_of(layer, ins, outs, scratch):
        return pl.pallas_call(
            functools.partial(root_kernel, layer),
            grid_spec=pltpu.PrefetchScalarGridSpec(
                num_scalar_prefetch=3,
                grid=(1,),
                in_specs=[RESIDENT] * len(ins),
                out_specs=[RESIDENT] * len(outs),
                scratch_shapes=[pltpu.VMEM(*each) for each in scratch],
            ),
            out_shape=[pltpu.VMEM(*each) for each in outs],
            compiler_params=params(30),
        )(place, row_counts, block_owner, *[resident(value) for value in ins])

    (root_zero,) = root_of(0, sets[0], [(square, BF16)], scratch)
    root_zero = resident(root_zero)
    outs = [(strip, BF16)] * 3 + [((8, TILE), F32)]
    outs += [(square, BF16), (square, F32), (square, BF16), (square, BF16)]
    upper, own_upper, other_upper, *kept = root_of(
        1, sets[1] + [root_zero], outs, [(square, F32), (square, BF16)]
    )
    back_upper = resident(swapped(other_upper))
    lower_half = pl.pallas_call(
        lower_kernel,
        grid_spec=pltpu.PrefetchScalarGridSpec(
            num_scalar_prefetch=2,
            grid=(1,),
            in_specs=[RESIDENT] * 6,
            out_specs=[RESIDENT] * 3,
        ),
        out_shape=[pltpu.VMEM(strip, BF16)] * 3,
        compiler_params=params(12),
        cost_estimate=products(STEP * BLOCK * BLOCK),
        name="lower",
    )
    kept = [resident(value) for value in kept]
    lower, own_lower, other_lower = lower_half(place, block_owner, root_zero, *kept)
    back_lower = resident(swapped(other_lower))
    roots = (root_zero, resident(upper), resident(lower))

    def update_of(other_core, rows, spec):
        return pl.pallas_call(
            functools.partial(update_kernel, other_core),
            grid_spec=pltpu.PrefetchScalarGridSpec(
                num_scalar_prefetch=2,
                grid=(1,),
                in_specs=[spec] + [RESIDENT] * 3,
                out_specs=RESIDENT,
            ),
            out_shape=pltpu.VMEM(parts, BF16),
            compiler_params=params(16),
            cost_estimate=products(row_slots * columns * BLOCK),
        )(place, row_counts, rows, *roots)

    update_other = update_of(True, other, RESIDENT)
    update_back = resident(swapped(update_other))
    own_columns = pl.BlockSpec(parts, lambda i, p, c: (0, 0, p[CORE]))
    update_own = resident(update_of(False, gradients, own_columns))
    anywhere = pl.BlockSpec(memory_space=pl.ANY)
    return pl.pallas_call(
        finish_kernel,
        grid_spec=pltpu.PrefetchScalarGridSpec(
            num_scalar_prefetch=2,
            grid=(1,),
            in_specs=[RESIDENT] * 6,
            out_specs=[anywhere, anywhere],
            scratch_shapes=[pltpu.SemaphoreType.DMA((6,))],
        ),
        out_shape=[
            jax.ShapeDtypeStruct(gradients.shape, BF16),
            jax.ShapeDtypeStruct(square, BF16),
        ],
        compiler_params=params(4),
        name="finish",
    )(
        place,
        block_owner,
        update_own,
        update_back,
        resident(own_upper),
        resident(own_lower),
        back_upper,
        back_lower,
    )


def solution(mesh):
    cores = Mesh(mesh.devices.reshape(SIDE, SIDE, 2, SIDE), ROWS + ("tp",))
    return jax.shard_map(
        body,
        mesh=cores,
        in_specs=(P(None, ROWS, "tp"), P(), P()),
        out_specs=(P(None, ROWS, "tp"), P(ROWS, "tp")),
        check_vma=False,
    )
```

```python
import functools

import jax
import jax.numpy as jnp
from jax import lax
from jax.experimental import pallas as pl
from jax.experimental.pallas import tpu as pltpu
from jax.sharding import Mesh, PartitionSpec as P


BLOCK = 1024
TILE = 128
HALF = 64
WIDE = 640
SIDE = 4
LAYERS = 2
STEP = 1024
damping = 0.01
F32 = jnp.float32
BF16 = jnp.bfloat16


def params(mebibytes):
    return pltpu.CompilerParams(vmem_limit_bytes=mebibytes * 1024 * 1024)


RESIDENT = pl.BlockSpec(memory_space=pltpu.VMEM)
LINE = (SIDE, HALF, WIDE)
PAIR = (LAYERS, HALF, WIDE)
Z, X, CORE, TP = range(4)
OUT = (0, 2, 1, 3)
BACK = (0, 1, 3, 2)
ROWS = ("z", "x", "core")


def valid_rows(place, counts, who, value):
    rows = lax.broadcasted_iota(jnp.int32, value.shape, 0)
    limit = counts[(place[Z] * SIDE + place[X]) * 2 + who]
    return jnp.where(rows < limit, value, jnp.zeros_like(value))


def chunk_of(place, first, second):
    z = second + place[CORE] * (first - second)
    x = first + place[CORE] * (second - first)
    return ((place[Z] + z) % SIDE) * SIDE + (place[X] + x) % SIDE


def away_kernel(place, half, out):
    out[pl.program_id(0)] = half[0]


def gram_kernel(place, counts, own, other, *refs):
    outs, (wide, gram) = refs[:SIDE], refs[SIDE:]
    rows = own.shape[1]
    for layer in range(LAYERS):
        wide[:rows, :BLOCK] = valid_rows(place, counts, place[CORE], own[layer])
        wide[rows:, :BLOCK] = valid_rows(place, counts, 1 - place[CORE], other[layer])
        wide[:, BLOCK:] = wide[:, : BLOCK // 2]
        for pair in range(4):
            start = pair * 2 * TILE
            part = lax.dot_general(
                wide[:, start : start + 2 * TILE],
                wide[:, start : start + 6 * TILE],
                (((0,), (0,)), ((), ())),
                preferred_element_type=F32,
            )
            for quarter in range(4):
                shift = TILE * (quarter // 2)
                gram[4 * pair + quarter] = part[
                    quarter * HALF : (quarter + 1) * HALF, shift : shift + WIDE
                ]
        for first in range(SIDE):
            for second in range(SIDE):
                value = gram[chunk_of(place, first, second)]
                outs[first][layer, second] = value.astype(outs[first].dtype)


def first_sum_kernel(*refs):
    ins, outs = refs[:SIDE], refs[SIDE:]
    for layer in range(LAYERS):
        for second in range(SIDE):
            value = ins[0][layer, second]
            for k in range(1, SIDE):
                value = value + ins[k][layer, second].astype(F32)
            outs[second][layer] = value.astype(outs[second].dtype)


def second_sum_kernel(*refs):
    value = refs[0][...]
    for k in range(1, SIDE):
        value = value + refs[k][...].astype(F32)
    refs[SIDE][...] = value.astype(BF16)


def line_kernel(*refs):
    for layer in range(LAYERS):
        for k in range(SIDE):
            refs[SIDE + layer][BACK[k]] = refs[k][layer]


def diagonal(start, rows):
    row = lax.broadcasted_iota(jnp.int32, (rows, BLOCK), 0) + start
    return row == lax.broadcasted_iota(jnp.int32, (rows, BLOCK), 1)


def root_kernel(layer, place, counts, owners, *refs):
    sets, refs = refs[:4], refs[4:]
    if layer == 1:
        before, refs = refs[0], refs[1:]
    root, refs = refs[0], refs[1:]
    if layer == 1:
        (root_own, root_other), refs = refs[:2], refs[2:]
    g_ref, w_ref, v_ref, rb_ref, wb_ref, vb_ref = refs

    for slot, first in enumerate(BACK):
        for second in range(SIDE):
            chunk = chunk_of(place, first, second)
            row = pl.multiple_of(chunk * HALF, HALF)
            value = sets[slot][second]
            for k in range(WIDE // TILE):
                column = pl.multiple_of(((chunk // 2 + k) % 8) * TILE, TILE)
                g_ref[pl.ds(row, HALF), pl.ds(column, TILE)] = value[:, k * TILE : (k + 1) * TILE]

    for slab in range(8):
        for k in range(1, 4):
            far = (slab + k) % 8
            here = slice(slab * TILE, (slab + 1) * TILE)
            there = slice(far * TILE, (far + 1) * TILE)
            g_ref[there, here] = g_ref[here, there].T

    squares = jnp.zeros((1, BLOCK), F32)
    trace = jnp.zeros((1, TILE), F32)
    row = lax.broadcasted_iota(jnp.int32, (TILE, TILE), 0)
    corner = row == lax.broadcasted_iota(jnp.int32, (TILE, TILE), 1)
    for slab in range(8):
        here = slice(slab * TILE, (slab + 1) * TILE)
        value = g_ref[here, :].astype(F32)
        squares = squares + jnp.sum(value * value, axis=0, keepdims=True)
        value = jnp.where(corner, g_ref[here, here].astype(F32), 0.0)
        trace = trace + jnp.sum(value, axis=0, keepdims=True)
    squares = jnp.sum(squares, axis=1, keepdims=True)
    trace = jnp.sum(trace, axis=1, keepdims=True)
    total = counts[0]
    for k in range(1, counts.shape[0]):
        total = total + counts[k]
    inverse = 1.0 / jnp.full((1, 1), total, jnp.int32).astype(F32)
    norm = squares * inverse * inverse + 2.0 * damping * inverse * trace
    scaling = 2.5 / jnp.sqrt(norm + damping * damping * BLOCK)
    a = scaling * inverse
    b = scaling * damping
    r_g, r_p, r_i = a * (10.0 - 2.0 * b) / 16.0, a * a / 16.0, b * (10.0 - b) / 16.0
    w_g, w_p, w_i = a * (5.0 - 2.0 * b) / 4.0, a * a / 4.0, b * (5.0 - b) / 4.0
    for part in range(BLOCK // STEP):
        here = slice(part * STEP, (part + 1) * STEP)
        product = jnp.dot(g_ref[here, :], g_ref[...], preferred_element_type=F32)
        value = g_ref[here, :].astype(F32)
        on = diagonal(part * STEP, STEP)
        rb_ref[here, :] = (r_g * value - r_p * product + jnp.where(on, r_i, 0.0)).astype(BF16)
        inner = w_g * value - w_p * product + jnp.where(on, w_i, 0.0)
        w_ref[here, :] = inner
        wb_ref[here, :] = inner.astype(BF16)
    for part in range(BLOCK // STEP):
        here = slice(part * STEP, (part + 1) * STEP)
        product = jnp.dot(rb_ref[here, :], wb_ref[...], preferred_element_type=F32)
        inner = (25.0 / 16.0) * w_ref[here, :] - product
        v_ref[here, :] = inner
        vb_ref[here, :] = inner.astype(BF16)
    quarter = jnp.sqrt(jnp.sqrt(scaling)) * 0.25
    for part in range(BLOCK // STEP):
        here = slice(part * STEP, (part + 1) * STEP)
        product = jnp.dot(rb_ref[here, :], vb_ref[...], preferred_element_type=F32)
        inner = product - (25.0 / 16.0) * v_ref[here, :]
        on = diagonal(part * STEP, STEP)
        inner = inner - (1.25 * a) * g_ref[here, :].astype(F32)
        inner = inner + jnp.where(on, 6.25 - 1.25 * b, 0.0)
        root[here, :] = (quarter * inner).astype(BF16)

    if layer == 0:
        return
    index = (place[Z] * SIDE + place[X]) * 2
    for target, who in ((root_own, place[CORE]), (root_other, 1 - place[CORE])):
        target[...] = jnp.zeros_like(target)
        for k, source in enumerate((before, root)):

            @pl.when(owners[k, place[TP] * 2 + place[CORE]] == index + who)
            def _():
                target[...] = source[...]


def update_kernel(other_core, place, counts, rows, root_zero, root_one, update):
    who = 1 - place[CORE] if other_core else place[CORE]
    for layer, root in enumerate((root_zero, root_one)):
        value = valid_rows(place, counts, who, rows[layer])
        product = jnp.dot(value, root[...], preferred_element_type=F32)
        update[layer] = product.astype(BF16)


def finish_kernel(place, owners, own, back, root_own, root_back, update, owned, sems):
    core = place[CORE]
    copies = []
    half = own.shape[1] // 2
    for source, side in ((own, core), (back, 1 - core)):
        columns = pl.ds(pl.multiple_of(side * BLOCK, BLOCK), BLOCK)
        for layer in range(LAYERS):
            for rows in (pl.ds(0, half), pl.ds(half, half)):
                target = update.at[layer, rows, columns]
                sem = sems.at[len(copies)]
                copies.append(pltpu.make_async_copy(source.at[layer, rows], target, sem))
    for copy in copies:
        copy.start()
    index = (place[Z] * SIDE + place[X]) * 2 + core
    column = place[TP] * 2 + core
    mine = jnp.logical_or(owners[0, column] == index, owners[1, column] == index)

    def write(source, first):
        quarter = BLOCK // 4
        parts = []
        for k in range(4):
            rows = pl.ds(k * quarter, quarter)
            parts.append(pltpu.make_async_copy(source.at[rows], owned.at[rows], sems.at[first + k]))
        for copy in parts:
            copy.start()
        for copy in parts:
            copy.wait()

    @pl.when(mine)
    def _():
        write(root_own, 8)

    @pl.when(jnp.logical_not(mine))
    def _():
        write(root_back, 12)

    for copy in copies:
        copy.wait()


def shifted(value, outer, distance):
    pairs = []
    for z in range(SIDE):
        for x in range(SIDE):
            for core in range(2):
                if outer == (core == 0):
                    there = (z, (x + distance) % SIDE)
                else:
                    there = ((z + distance) % SIDE, x)
                pairs.append(
                    ((z * SIDE + x) * 2 + core, (there[0] * SIDE + there[1]) * 2 + core)
                )
    return lax.ppermute(value, ROWS, pairs)


def swapped(value):
    return lax.ppermute(value, "core", [(0, 1), (1, 0)])


def resident(value):
    return pltpu.with_memory_space_constraint(value, pltpu.VMEM)


def local_call(kernel, name, ins, outs):
    return pl.pallas_call(
        kernel,
        in_specs=[RESIDENT] * len(ins),
        out_specs=[RESIDENT] * len(outs),
        out_shape=[pltpu.VMEM(*each) for each in outs],
        compiler_params=params(4),
        name=name,
    )(*[resident(value) for value in ins])


def body(gradients, row_counts, block_owner):
    place = jnp.stack([lax.axis_index(name) for name in ("z", "x", "core", "tp")])
    place = place.astype(jnp.int32)
    _, row_slots, _ = gradients.shape
    square = (BLOCK, BLOCK)
    part = (row_slots, BLOCK)
    parts = (LAYERS,) + part

    away = pl.pallas_call(
        away_kernel,
        grid_spec=pltpu.PrefetchScalarGridSpec(
            num_scalar_prefetch=1,
            grid=(LAYERS,),
            in_specs=[pl.BlockSpec((1,) + part, lambda k, p: (k, 0, 1 - p[CORE]))],
            out_specs=RESIDENT,
        ),
        out_shape=pltpu.VMEM(parts, BF16),
        compiler_params=params(8),
        name="away",
    )(place, pltpu.with_memory_space_constraint(gradients, pltpu.HBM))
    other = resident(swapped(away))

    grams = pl.pallas_call(
        gram_kernel,
        grid_spec=pltpu.PrefetchScalarGridSpec(
            num_scalar_prefetch=2,
            grid=(1,),
            in_specs=[pl.BlockSpec(parts, lambda i, p, c: (0, 0, p[CORE])), RESIDENT],
            out_specs=[RESIDENT] * SIDE,
            scratch_shapes=[
                pltpu.VMEM((2 * row_slots, BLOCK + BLOCK // 2), BF16),
                pltpu.VMEM((16, HALF, WIDE), F32),
            ],
        ),
        out_shape=[pltpu.VMEM((LAYERS,) + LINE, BF16 if k else F32) for k in range(SIDE)],
        compiler_params=params(20),
        name="gram",
    )(place, row_counts, gradients, other)

    def exchange(values, outer, sign):
        return [values[0]] + [shifted(values[k], outer, sign * k) for k in (OUT if sign > 0 else BACK)[1:]]

    outs = [(PAIR, BF16 if k else F32) for k in range(SIDE)]
    summed = local_call(first_sum_kernel, "first", exchange(grams, True, 1), outs)
    summed = exchange(summed, False, 1)
    (reduced,) = local_call(second_sum_kernel, "second", summed, [(PAIR, BF16)])
    pieces = exchange([reduced] * SIDE, False, -1)
    lines = local_call(line_kernel, "line", pieces, [(LINE, BF16)] * LAYERS)
    sets = [exchange([line] * SIDE, True, -1) for line in lines]

    def root_of(layer, ins, outs):
        return pl.pallas_call(
            functools.partial(root_kernel, layer),
            grid_spec=pltpu.PrefetchScalarGridSpec(
                num_scalar_prefetch=3,
                grid=(1,),
                in_specs=[RESIDENT] * len(ins),
                out_specs=[RESIDENT] * outs,
                scratch_shapes=[
                    pltpu.VMEM(square, BF16),
                    pltpu.VMEM(square, F32),
                    pltpu.VMEM(square, F32),
                    pltpu.VMEM(square, BF16),
                    pltpu.VMEM(square, BF16),
                    pltpu.VMEM(square, BF16),
                ],
            ),
            out_shape=[pltpu.VMEM(square, BF16)] * outs,
            compiler_params=params(30),
            name=f"root_{layer}",
        )(place, row_counts, block_owner, *[resident(value) for value in ins])

    root_zero = resident(root_of(0, sets[0], 1)[0])
    root_one, root_own, root_other = root_of(1, sets[1] + [root_zero], 3)
    root_back = resident(swapped(root_other))
    roots = (root_zero, resident(root_one))

    def update_of(other_core, rows, spec, name):
        return pl.pallas_call(
            functools.partial(update_kernel, other_core),
            grid_spec=pltpu.PrefetchScalarGridSpec(
                num_scalar_prefetch=2,
                grid=(1,),
                in_specs=[spec, RESIDENT, RESIDENT],
                out_specs=RESIDENT,
            ),
            out_shape=pltpu.VMEM(parts, BF16),
            compiler_params=params(16),
            name=name,
        )(place, row_counts, rows, *roots)

    update_back = resident(swapped(update_of(True, other, RESIDENT, "update_other")))
    own_columns = pl.BlockSpec(parts, lambda i, p, c: (0, 0, p[CORE]))
    update_own = resident(update_of(False, gradients, own_columns, "update_own"))
    anywhere = pl.BlockSpec(memory_space=pl.ANY)
    return pl.pallas_call(
        finish_kernel,
        grid_spec=pltpu.PrefetchScalarGridSpec(
            num_scalar_prefetch=2,
            grid=(1,),
            in_specs=[RESIDENT] * 4,
            out_specs=[anywhere, anywhere],
            scratch_shapes=[pltpu.SemaphoreType.DMA((16,))],
        ),
        out_shape=[
            jax.ShapeDtypeStruct(gradients.shape, BF16),
            jax.ShapeDtypeStruct(square, BF16),
        ],
        compiler_params=params(4),
        name="finish",
    )(place, block_owner, update_own, update_back, resident(root_own), root_back)


def solution(mesh):
    cores = Mesh(mesh.devices.reshape(SIDE, SIDE, 2, SIDE), ROWS + ("tp",))
    return jax.shard_map(
        body,
        mesh=cores,
        in_specs=(P(None, ROWS, "tp"), P(), P()),
        out_specs=(P(None, ROWS, "tp"), P(ROWS, "tp")),
        check_vma=False,
    )
```
